64 devices in a mesh: dp: 8 (over x, y, core), sp: 8 (over z).
Axes of the slice: x: 2, y: 2, z: 8, core: 2. Of those that a mesh axis runs over, the one named last changes fastest.
The devices are a block of a 4x4x8 slice.
Arguments:
- x: bfloat16 [16384, 5120], P(('dp', 'sp')), parts along dimension 0
- gain: bfloat16 [5120], replicated
- wq: bfloat16 [5120, 12288], replicated
- wk: bfloat16 [5120, 1024], replicated
- wv: bfloat16 [5120, 1024], replicated
- wo: bfloat16 [12288, 5120], replicated
Outputs:
- output: bfloat16 [16384, 5120], P(('dp', 'sp')), parts along dimension 0
There are 8 independent parts. The reference program is written for one: setup_inputs(seed, part) draws one part's arguments, and reference() takes and returns one part's arrays. A program takes and returns all parts, laid end to end along the dimension named above; an argument that names none is the same for every part.
All inputs are finite; a program needn't handle non-finite values.
Results may differ from the reference program's by a relative error of at most 0.012.
Values are sent between devices in bfloat16 or wider.
A program may use at most 768 MiB of HBM per device.

```python
import jax
import jax.numpy as jnp
from jax import lax

ROWS = 2048
D = 5120
HEADS = 96
KV_HEADS = 8
HEAD = 128
THETA = 10000


def setup_inputs(seed: int = 0, part: int = 0) -> dict:
    kx, kn, kq, kk, kv, ko = jax.random.split(jax.random.key(seed), 6)

    def weights(key, rows, columns):
        return jax.random.normal(key, (rows, columns), jnp.float32) * rows**-0.5

    drawn = {
        "x": jax.random.normal(jax.random.fold_in(kx, part), (ROWS, D), jnp.float32),
        "gain": 1 + 0.1 * jax.random.normal(kn, (D,), jnp.float32),
        "wq": 2 * weights(kq, D, HEADS * HEAD),
        "wk": 2 * weights(kk, D, KV_HEADS * HEAD),
        "wv": 4 * weights(kv, D, KV_HEADS * HEAD),
        "wo": weights(ko, HEADS * HEAD, D),
    }
    return {k: v.astype(jnp.bfloat16) for k, v in drawn.items()}


def normed(x, gain):
    wide = x.astype(jnp.float32)
    scale = lax.rsqrt(jnp.mean(wide * wide, -1, keepdims=True) + 1e-6)
    return (wide * scale * gain.astype(jnp.float32)).astype(jnp.bfloat16)


def turned(t, place, theta):
    half = t.shape[-1] // 2
    angle = place.astype(jnp.float32)[:, None] * theta ** (-jnp.arange(half, dtype=jnp.float32) / half)
    cos, sin = jnp.cos(angle)[:, None], jnp.sin(angle)[:, None]
    a, b = t[..., :half].astype(jnp.float32), t[..., half:].astype(jnp.float32)
    return jnp.concatenate([a * cos - b * sin, b * cos + a * sin], -1).astype(jnp.bfloat16)


def matmul(a, w):
    return jnp.dot(a, w, preferred_element_type=jnp.float32).astype(jnp.bfloat16)


def einsum(form, a, b):
    return jnp.einsum(form, a.astype(jnp.float32), b.astype(jnp.float32))


def attention(q, k, v):
    scores = einsum("tgsd,ugd->gstu", q, k) * q.shape[-1] ** -0.5
    token = jnp.arange(q.shape[0])
    scores = jnp.where(token[:, None] >= token, scores, -jnp.inf)
    weights = jax.nn.softmax(scores, -1).astype(jnp.bfloat16)
    return einsum("gstu,ugd->tgsd", weights, v).astype(jnp.bfloat16)


def reference(x, gain, wq, wk, wv, wo):
    a, place = normed(x, gain), jnp.arange(ROWS)
    q = turned(matmul(a, wq).reshape(ROWS, HEADS, HEAD), place, THETA).reshape(ROWS, KV_HEADS, -1, HEAD)
    k = turned(matmul(a, wk).reshape(ROWS, KV_HEADS, HEAD), place, THETA)
    v = matmul(a, wv).reshape(ROWS, KV_HEADS, HEAD)
    seen = attention(q, k, v).reshape(ROWS, HEADS * HEAD)
    return (x.astype(jnp.float32) + jnp.dot(seen, wo, preferred_element_type=jnp.float32)).astype(jnp.bfloat16)
```

```python
import functools

import jax
import jax.numpy as jnp
from jax import lax
from jax.experimental import pallas as pl
from jax.experimental.pallas import tpu as pltpu
from jax.sharding import PartitionSpec as P

HEAD = 128
THETA = 10000
LOG2E = 1.4426950408889634
HIDDEN = -2e30
MESH = pl.DeviceIdType.MESH
VMEM_LIMIT = 62 * 2**20


def _dot(a, b, ca=1, cb=0):
    return lax.dot_general(a, b, (((ca,), (cb,)), ((), ())), preferred_element_type=jnp.float32)


def _turn(t, cos, sin):
    return (t * cos + pltpu.roll(t, HEAD // 2, 1) * sin).astype(jnp.bfloat16)


def _kv_kernel(x_ref, gain_ref, wk_ref, wv_ref, cos_ref, sin_ref, a_ref, kv_ref):
    own = x_ref.shape[0]

    @pl.when(pl.program_id(0) == 0)
    def _():
        rows = 32
        for r in range(0, own, rows):
            wide = x_ref[r : r + rows, :].astype(jnp.float32)
            scale = lax.rsqrt(jnp.mean(wide * wide, -1, keepdims=True) + 1e-6)
            a_ref[r : r + rows, :] = (wide * scale * gain_ref[...].astype(jnp.float32)).astype(jnp.bfloat16)

    a = a_ref[...]
    k = _dot(a, wk_ref[...]).astype(jnp.bfloat16).astype(jnp.float32)
    v = _dot(a, wv_ref[...]).astype(jnp.bfloat16).astype(jnp.float32)
    cos, sin = cos_ref[...], sin_ref[...]
    for h in range(kv_ref.shape[0]):
        here = slice(h * HEAD, (h + 1) * HEAD)
        kv_ref[h, :own, :] = _turn(k[:, here], cos, sin)
        vt = v[:, here].T.astype(jnp.bfloat16)
        for part in range(own // HEAD):
            kv_ref[h, own + part * HEAD : own + (part + 1) * HEAD, :] = vt[:, part * HEAD : (part + 1) * HEAD]


def project_kv(x, gain, wk, wv, cos, sin):
    own, d = x.shape
    heads, per = wk.shape[1] // HEAD, 2
    full = lambda *s: pl.BlockSpec(s, lambda i: (0,) * len(s))
    weight = pl.BlockSpec((d, per * HEAD), lambda i: (0, i))
    return pl.pallas_call(
        _kv_kernel,
        name="project_kv",
        grid=(heads // per,),
        in_specs=[full(own, d), full(1, d), weight, weight, full(own, HEAD), full(own, HEAD)],
        out_specs=[full(own, d), pl.BlockSpec((per, 2 * own, HEAD), lambda i: (i, 0, 0))],
        out_shape=[jax.ShapeDtypeStruct((own, d), jnp.bfloat16), jax.ShapeDtypeStruct((heads, 2 * own, HEAD), jnp.bfloat16)],
        compiler_params=pltpu.CompilerParams(vmem_limit_bytes=VMEM_LIMIT, dimension_semantics=("arbitrary",)),
        cost_estimate=pl.CostEstimate(flops=4 * own * d * heads * HEAD, bytes_accessed=4 * d * heads * HEAD, transcendentals=0),
    )(x, gain.reshape(1, d), wk, wv, cos, sin)


class Ring:
    def __init__(self, n, kv, send, recv):
        self.n, self.kv, self.send, self.recv = n, kv, send, recv
        self.me = lax.axis_index("sp")
        self.ticks = kv.shape[0] // 2 * 7

    def copy(self, way, h, s, block):
        to = lax.rem(self.me + (1 if way == 0 else self.n - 1), self.n)
        ref = self.kv.at[h, block]
        return pltpu.make_async_remote_copy(
            src_ref=ref, dst_ref=ref, send_sem=self.send.at[way, h, s], recv_sem=self.recv.at[way, h, s],
            device_id={"sp": to}, device_id_type=MESH)

    def sent(self, way, h, s):
        return self.copy(way, h, s, lax.rem(self.me + (self.n - s if way == 0 else s), self.n))

    def got(self, way, h, s):
        return self.copy(way, h, s, lax.rem(self.me + (self.n - s - 1 if way == 0 else s + 1), self.n))

    def tick(self, t):
        pair, r = t // 7, lax.rem(t, 7)
        s = r // 2
        for way in (0, 1):
            odd = lax.rem(r, 2)
            h = pair * 2 + (odd if way == 0 else 1 - odd)

            @pl.when(s > 0)
            def _():
                self.got(way, h, jnp.maximum(s - 1, 0)).wait_recv()

            self.sent(way, h, s).start()

    def arrive(self, h):
        odd = lax.rem(h, 2)
        self.got(0, h, 3 - odd).wait_recv()
        self.got(1, h, 2 + odd).wait_recv()

    def drain(self):
        def body(h, _):
            odd = lax.rem(h, 2)
            for way in (0, 1):
                for s in range(3):
                    self.sent(way, h, s).wait_send()

            @pl.when(odd == 0)
            def _():
                self.sent(0, h, 3).wait_send()

            @pl.when(odd == 1)
            def _():
                self.sent(1, h, 3).wait_send()

        lax.fori_loop(0, self.kv.shape[0], body, None)


def _pair(blocks, own, kv, q_ref, gap_ref, new, cur, o_ref, i, pairs, per, scale):
    (s_new, m_new, a_new), (s_cur, m_cur, a_cur) = new, cur
    e = scale * LOG2E
    ahead, here, back = jnp.minimum(i, pairs - 1), jnp.clip(i - 1, 0, pairs - 1), jnp.maximum(i - 2, 0)
    g_ahead, g_here = ahead // per, here // per
    q = q_ref[pl.ds(ahead * 2, 2)].reshape(2 * own, HEAD)
    top = m_cur[...].max(0, keepdims=True)
    ones = jnp.ones((8, own), jnp.bfloat16)

    done = a_new[...]
    out = (done[:HEAD] * (1 / done[HEAD : HEAD + 1])).T.astype(jnp.bfloat16)
    o_ref[:, pl.ds(pl.multiple_of(back * 2 * HEAD, 2 * HEAD), HEAD)] = out[:own]
    o_ref[:, pl.ds(pl.multiple_of(back * 2 * HEAD + HEAD, HEAD), HEAD)] = out[own:]

    most = total = None
    for b in range(blocks):
        s = _dot(kv[g_ahead, b, :own, :], q, 1, 1)
        if b == blocks - 1:
            s = jnp.where(gap_ref[...] >= 0, s, HIDDEN)
        s_new[b * own : (b + 1) * own, :] = s
        high = s.reshape(own // 8, 8, 2 * own).max(0)
        most = high if most is None else jnp.maximum(most, high)
        p = jnp.exp2((s_cur[b * own : (b + 1) * own, :] - top) * e).astype(jnp.bfloat16)
        values = jnp.concatenate([kv[g_here, b, own + c : own + c + HEAD, :] for c in range(0, own, HEAD)], axis=1)
        part = _dot(jnp.concatenate([values, ones], axis=0), p)
        total = part if total is None else total + part
    m_new[...] = most
    a_cur[...] = total


def _attend_kernel(a_hbm, kv_hbm, wq_hbm, cos_ref, sin_ref, o_ref, kv, a_ref, w_ref, q_ref, s0, s1, m0, m1, a0, a1, gap,
                   send, recv, w_sem, in_sem, *, n, tile):
    me = lax.axis_index("sp")
    own, d = a_ref.shape
    heads = q_ref.shape[0]
    key_heads = kv.shape[0]
    pairs, per = heads // 2, heads // 2 // key_heads
    steps = wq_hbm.shape[1] // tile
    scale = HEAD**-0.5

    def weight(i):
        slot = lax.rem(i, 2)
        return pltpu.make_async_copy(wq_hbm.at[:, pl.ds(pl.multiple_of(i * tile, tile), tile)], w_ref.at[slot], w_sem.at[slot])

    mine = pltpu.make_async_copy(kv_hbm, kv.at[:, me], in_sem.at[0])
    mine.start()
    states = pltpu.make_async_copy(a_hbm, a_ref, in_sem.at[1])
    states.start()
    weight(0).start()
    weight(1).start()

    barrier = pltpu.get_barrier_semaphore()
    for to in (lax.rem(me + 1, n), lax.rem(me + n - 1, n)):
        pl.semaphore_signal(barrier, inc=1, device_id={"sp": to}, device_id_type=MESH)
    pl.semaphore_wait(barrier, 2)

    ring = Ring(n, kv, send, recv)
    mine.wait()
    ring.tick(0)
    ring.tick(1)
    states.wait()

    gap[...] = lax.rem(lax.broadcasted_iota(jnp.int32, gap.shape, 1), own) - lax.broadcasted_iota(jnp.int32, gap.shape, 0)
    s1[...] = jnp.zeros_like(s1)
    m1[...] = jnp.zeros_like(m1)
    a0[...] = jnp.ones_like(a0)
    a1[...] = jnp.ones_like(a1)

    def project(i, _):
        ring.tick(i + 2)
        weight(i).wait()
        t = _dot(a_ref[...], w_ref[lax.rem(i, 2)]).astype(jnp.bfloat16).astype(jnp.float32)
        cos, sin = cos_ref[...], sin_ref[...]
        for h in range(tile // HEAD):
            q_ref[i * (tile // HEAD) + h] = _turn(t[:, h * HEAD : (h + 1) * HEAD], cos, sin)

        @pl.when(i + 2 < steps)
        def _():
            weight(i + 2).start()

    lax.fori_loop(0, steps, project, None)

    even, odd = (s0, m0, a0), (s1, m1, a1)

    def attend(i, _):
        @pl.when((lax.rem(i, per) == 0) & (i < pairs))
        def _():
            ring.arrive(i // per)

        at = steps + 2 + i // 2

        @pl.when((lax.rem(i, 2) == 0) & (at < ring.ticks))
        def _():
            ring.tick(at)

        for blocks in range(1, n + 1):
            for parity, (new, cur) in enumerate(((even, odd), (odd, even))):

                @pl.when((me == blocks - 1) & (lax.rem(i, 2) == parity))
                def _():
                    _pair(blocks, own, kv, q_ref, gap, new, cur, o_ref, i, pairs, per, scale)

    lax.fori_loop(0, pairs + 2, attend, None)
    ring.drain()


def attend(a, kv, wq, cos, sin, n):
    own, d = a.shape
    key_heads = kv.shape[0]
    heads = wq.shape[1] // HEAD
    tile = 1024
    state = lambda *s: [pltpu.VMEM(s, jnp.float32)] * 2
    hbm, vmem = pl.BlockSpec(memory_space=pl.ANY), pl.BlockSpec(memory_space=pltpu.VMEM)
    return pl.pallas_call(
        functools.partial(_attend_kernel, n=n, tile=tile),
        name="attend",
        in_specs=[hbm, hbm, hbm, vmem, vmem],
        out_specs=vmem,
        out_shape=jax.ShapeDtypeStruct((own, heads * HEAD), jnp.bfloat16),
        scratch_shapes=[
            pltpu.VMEM((key_heads, n, 2 * own, HEAD), jnp.bfloat16),
            pltpu.VMEM((own, d), jnp.bfloat16),
            pltpu.VMEM((2, d, tile), jnp.bfloat16),
            pltpu.VMEM((heads, own, HEAD), jnp.bfloat16),
            *state(n * own, 2 * own),
            *state(8, 2 * own),
            *state(HEAD + 8, 2 * own),
            pltpu.VMEM((own, 2 * own), jnp.int32),
            pltpu.SemaphoreType.DMA((2, key_heads, 4)),
            pltpu.SemaphoreType.DMA((2, key_heads, 4)),
            pltpu.SemaphoreType.DMA((2,)),
            pltpu.SemaphoreType.DMA((2,)),
        ],
        compiler_params=pltpu.CompilerParams(vmem_limit_bytes=VMEM_LIMIT, collective_id=0, has_side_effects=True),
        cost_estimate=pl.CostEstimate(flops=2 * own * d * heads * HEAD, bytes_accessed=2 * d * heads * HEAD, transcendentals=0),
    )(a, kv, wq, cos, sin)


def _out_kernel(o_ref, w_ref, x_ref, y_ref, acc):
    c = pl.program_id(0)
    part = _dot(o_ref[...], w_ref[...])

    @pl.when(c == 0)
    def _():
        acc[...] = part

    @pl.when((c > 0) & (c < pl.num_programs(0) - 1))
    def _():
        acc[...] += part

    @pl.when(c == pl.num_programs(0) - 1)
    def _():
        y_ref[...] = (x_ref[...].astype(jnp.float32) + (acc[...] + part)).astype(jnp.bfloat16)


def project_out(o, wo, x):
    own, d = x.shape
    tile = 512
    return pl.pallas_call(
        _out_kernel,
        name="project_out",
        grid=(wo.shape[0] // tile,),
        in_specs=[pl.BlockSpec((own, tile), lambda c: (0, c)), pl.BlockSpec((tile, d), lambda c: (c, 0)), pl.BlockSpec((own, d), lambda c: (0, 0))],
        out_specs=pl.BlockSpec((own, d), lambda c: (0, 0)),
        out_shape=jax.ShapeDtypeStruct((own, d), jnp.bfloat16),
        scratch_shapes=[pltpu.VMEM((own, d), jnp.float32)],
        compiler_params=pltpu.CompilerParams(vmem_limit_bytes=VMEM_LIMIT, dimension_semantics=("arbitrary",)),
        cost_estimate=pl.CostEstimate(flops=2 * own * d * wo.shape[0], bytes_accessed=2 * d * wo.shape[0], transcendentals=0),
    )(o, wo, x)


def solution(mesh):
    n = mesh.shape["sp"]

    def step(x, gain, wq, wk, wv, wo):
        own = x.shape[0]
        half = HEAD // 2
        place = lax.axis_index("sp") * own + jnp.arange(own)
        angle = place.astype(jnp.float32)[:, None] * THETA ** (-jnp.arange(half, dtype=jnp.float32) / half)
        cos, sin = jnp.cos(angle), jnp.sin(angle)
        cos, sin = jnp.concatenate([cos, cos], -1), jnp.concatenate([-sin, sin], -1)
        a, kv = project_kv(x, gain, wk, wv, cos, sin)
        o = attend(a, kv, wq, cos, sin, n)
        return project_out(o, wo, x)

    tokens, whole = P(("dp", "sp"), None), P(None, None)
    return jax.shard_map(
        step, mesh=mesh, in_specs=(tokens, P(None), whole, whole, whole, whole), out_specs=tokens, check_vma=False)
```

```python
import functools

import jax
import jax.numpy as jnp
from jax import lax
from jax.experimental import pallas as pl
from jax.experimental.pallas import tpu as pltpu
from jax.sharding import PartitionSpec as P

HEAD = 128
THETA = 10000
LOG2E = 1.4426950408889634
HIDDEN = -2e30
MESH = pl.DeviceIdType.MESH
VMEM_LIMIT = 67_043_328


def _dot(a, b, ca=1, cb=0):
    return lax.dot_general(a, b, (((ca,), (cb,)), ((), ())), preferred_element_type=jnp.float32)


def _turn(t, cos, sin):
    return (t * cos + pltpu.roll(t, HEAD // 2, 1) * sin).astype(jnp.bfloat16)


class Ring:
    def __init__(self, n, kv, send, recv):
        self.n, self.kv, self.send, self.recv = n, kv, send, recv
        self.me = lax.axis_index("sp")
        self.ticks = kv.shape[0] // 2 * 7

    def copy(self, way, h, s, block):
        to = lax.rem(self.me + (1 if way == 0 else self.n - 1), self.n)
        ref = self.kv.at[h, block]
        return pltpu.make_async_remote_copy(
            src_ref=ref, dst_ref=ref, send_sem=self.send.at[way, h, s], recv_sem=self.recv.at[way, h, s],
            device_id={"sp": to}, device_id_type=MESH)

    def sent(self, way, h, s):
        return self.copy(way, h, s, lax.rem(self.me + (self.n - s if way == 0 else s), self.n))

    def got(self, way, h, s):
        return self.copy(way, h, s, lax.rem(self.me + (self.n - s - 1 if way == 0 else s + 1), self.n))

    def tick(self, t):
        pair, r = t // 7, lax.rem(t, 7)
        s = r // 2
        for way in (0, 1):
            odd = lax.rem(r, 2)
            h = pair * 2 + (odd if way == 0 else 1 - odd)

            @pl.when(s > 0)
            def _():
                self.got(way, h, jnp.maximum(s - 1, 0)).wait_recv()

            self.sent(way, h, s).start()

    def arrive(self, h):
        odd = lax.rem(h, 2)
        self.got(0, h, 3 - odd).wait_recv()
        self.got(1, h, 2 + odd).wait_recv()

    def drain(self):
        def body(h, _):
            odd = lax.rem(h, 2)
            for way in (0, 1):
                for s in range(3):
                    self.sent(way, h, s).wait_send()

            @pl.when(odd == 0)
            def _():
                self.sent(0, h, 3).wait_send()

            @pl.when(odd == 1)
            def _():
                self.sent(1, h, 3).wait_send()

        lax.fori_loop(0, self.kv.shape[0], body, None)


def _pair(blocks, own, kv, q_ref, gap_ref, new, cur, o_ref, i, pairs, per, scale):
    (s_new, m_new, a_new), (s_cur, m_cur, a_cur) = new, cur
    e = scale * LOG2E
    ahead, here, back = jnp.minimum(i, pairs - 1), jnp.clip(i - 1, 0, pairs - 1), jnp.maximum(i - 2, 0)
    g_ahead, g_here = ahead // per, here // per
    q = q_ref[pl.ds(ahead * 2, 2)].reshape(2 * own, HEAD)
    top = m_cur[...].max(0, keepdims=True)
    ones = jnp.ones((8, own), jnp.bfloat16)

    def scores(b, most):
        s = _dot(kv[g_ahead, b, :own, :], q, 1, 1)
        if b == blocks - 1:
            s = jnp.where(gap_ref[...] >= 0, s, HIDDEN)
        s_new[b * own : (b + 1) * own, :] = s
        high = s.reshape(own // 8, 8, 2 * own).max(0)
        return high if most is None else jnp.maximum(most, high)

    most, total = scores(0, None), None

    done = a_new[...]
    out = (done[:HEAD] * (1 / done[HEAD : HEAD + 1])).T.astype(jnp.bfloat16)
    o_ref[:, pl.ds(pl.multiple_of(back * 2 * HEAD, 2 * HEAD), HEAD)] = out[:own]
    o_ref[:, pl.ds(pl.multiple_of(back * 2 * HEAD + HEAD, HEAD), HEAD)] = out[own:]

    for b in range(blocks):
        if b + 1 < blocks:
            most = scores(b + 1, most)
        p = jnp.exp2((s_cur[b * own : (b + 1) * own, :] - top) * e).astype(jnp.bfloat16)
        values = jnp.concatenate([kv[g_here, b, own + c : own + c + HEAD, :] for c in range(0, own, HEAD)], axis=1)
        part = _dot(jnp.concatenate([values, ones], axis=0), p)
        total = part if total is None else total + part
    m_new[...] = most
    a_cur[...] = total


def _layer_kernel(x_hbm, gain_ref, wq_hbm, wk_hbm, wv_hbm, wo_hbm, freq_ref, y_hbm, kv, cos_ref, sin_ref, raw, x_ref, a_ref, w_ref, q_ref, o_ref,
                  s0, s1, m0, m1, a0, a1, gap, send, recv, w_sem, x_sem, y_sem, *, n):
    me = lax.axis_index("sp")
    own, d = x_ref.shape
    heads, key_heads = q_ref.shape[0], kv.shape[0]
    pairs, per = heads // 2, heads // 2 // key_heads
    tile = w_ref.shape[2]
    some = tile // HEAD
    kv_tiles, q_tiles = key_heads // some, heads // some
    narrow = tile // 2
    out_tiles = d // narrow

    def half(j):
        r = lax.rem(j, 4)
        return w_ref.at[r // 2, pl.ds(pl.multiple_of(lax.rem(r, 2) * d, d), d)]

    def load(w_hbm, i, j):
        return pltpu.make_async_copy(w_hbm.at[:, pl.ds(pl.multiple_of(i * tile, tile), tile)], half(j), w_sem.at[lax.rem(j, 4)])

    def half_out(c):
        r = lax.rem(c, 4)
        return w_ref.at[r // 2, :, pl.ds(pl.multiple_of(lax.rem(r, 2) * narrow, narrow), narrow)]

    def load_out(c):
        cols = pl.ds(pl.multiple_of(c * narrow, narrow), narrow)
        return pltpu.make_async_copy(wo_hbm.at[:, cols], half_out(c), w_sem.at[4 + lax.rem(c, 4)])

    states = pltpu.make_async_copy(x_hbm, x_ref, x_sem)
    states.start()
    first = [(w, i) for i in range(kv_tiles) for w in (wk_hbm, wv_hbm)]
    for j, (w, i) in enumerate(first):
        load(w, i, j).start()

    barrier = pltpu.get_barrier_semaphore()
    for to in (lax.rem(me + 1, n), lax.rem(me + n - 1, n)):
        pl.semaphore_signal(barrier, inc=1, device_id={"sp": to}, device_id_type=MESH)

    gap[...] = lax.rem(lax.broadcasted_iota(jnp.int32, gap.shape, 1), own) - lax.broadcasted_iota(jnp.int32, gap.shape, 0)
    m1[...] = jnp.zeros_like(m1)
    s1[...] = jnp.zeros_like(s1)
    a0[...] = jnp.ones_like(a0)
    a1[...] = jnp.ones_like(a1)
    place = (me * own + lax.broadcasted_iota(jnp.int32, cos_ref.shape, 0)).astype(jnp.float32)
    angle = place * freq_ref[0:1, :]
    cos_ref[...] = jnp.cos(angle)
    sin_ref[...] = jnp.where(lax.broadcasted_iota(jnp.int32, cos_ref.shape, 1) < HEAD // 2, -1.0, 1.0) * jnp.sin(angle)
    raw[...] = jnp.zeros_like(raw)
    gain = gain_ref[0:1, :]
    states.wait()

    def norm(r, _):
        for part in range(4):
            rows = pl.ds(pl.multiple_of(r * 64 + part * 16, 16), 16)
            wide = x_ref[rows, :].astype(jnp.float32)
            scale = lax.rsqrt(jnp.mean(wide * wide, -1, keepdims=True) + 1e-6)
            a_ref[rows, :] = (wide * scale * gain).astype(jnp.bfloat16)

    lax.fori_loop(0, own // 64, norm, None)
    pl.semaphore_wait(barrier, 2)
    ring = Ring(n, kv, send, recv)

    def product(j):
        r = lax.rem(j, 4)
        w = w_ref[r // 2, pl.ds(pl.multiple_of(lax.rem(r, 2) * d, d), d)]
        return _dot(a_ref[...], w).astype(jnp.bfloat16).astype(jnp.float32)

    for j, (w, i) in enumerate(first):
        load(w, i, j).wait()
        t = product(j)
        for h in range(some):
            one = t[:, h * HEAD : (h + 1) * HEAD]
            if w is wk_hbm:
                kv[i * some + h, me, :own, :] = _turn(one, cos_ref[...], sin_ref[...])
            else:
                vt = one.T.astype(jnp.bfloat16)
                for c in range(0, own, HEAD):
                    kv[i * some + h, me, own + c : own + c + HEAD, :] = vt[:, c : c + HEAD]
        load(wq_hbm, j, j + len(first)).start()
        if j == len(first) - 2:
            ring.tick(0)
            ring.tick(1)

    def turn(i):
        t = raw[...]
        for h in range(some):
            q_ref[i * some + h] = _turn(t[:, h * HEAD : (h + 1) * HEAD], cos_ref[...], sin_ref[...])

    early = 13

    def project(i, _):
        @pl.when(lax.rem(i * early, q_tiles) < early)
        def _():
            ring.tick(i * early // q_tiles + 2)

        j = i + len(first)
        load(wq_hbm, i, j).wait()
        turn(jnp.maximum(i - 1, 0))
        raw[...] = product(j)

        @pl.when(i + 4 < q_tiles)
        def _():
            load(wq_hbm, i + 4, j + 4).start()

    lax.fori_loop(0, q_tiles, project, None)
    for c in range(4):
        load_out(c).start()
    turn(q_tiles - 1)

    even, odd = (s0, m0, a0), (s1, m1, a1)

    def attend(i, _):
        @pl.when((lax.rem(i, per) == 0) & (i < pairs))
        def _():
            ring.arrive(i // per)

        at = early + 2 + i * 2 // 5

        @pl.when((lax.rem(i * 2, 5) < 2) & (at < ring.ticks))
        def _():
            ring.tick(at)

        for blocks in range(n, 0, -1):

            @pl.when(me == blocks - 1)
            def _():
                for parity, (new, cur) in enumerate(((even, odd), (odd, even))):

                    @pl.when(lax.rem(i, 2) == parity)
                    def _():
                        _pair(blocks, own, kv, q_ref, gap, new, cur, o_ref, i, pairs, per, HEAD**-0.5)

    lax.fori_loop(0, pairs + 2, attend, None)

    def columns(c):
        return pl.ds(pl.multiple_of(c * narrow, narrow), narrow)

    def store(c):
        return pltpu.make_async_copy(a_ref.at[:, columns(c)], y_hbm.at[:, columns(c)], y_sem.at[c])

    def add(c):
        a_ref[:, columns(c)] = (x_ref[:, columns(c)].astype(jnp.float32) + raw[:, :narrow]).astype(jnp.bfloat16)

    def out(c, _):
        load_out(c).wait()
        add(jnp.maximum(c - 1, 0))
        r = lax.rem(c, 4)
        raw[:, :narrow] = _dot(o_ref[...], w_ref[r // 2, :, pl.ds(pl.multiple_of(lax.rem(r, 2) * narrow, narrow), narrow)])

        @pl.when(c > 0)
        def _():
            store(jnp.maximum(c - 1, 0)).start()

        @pl.when(c + 4 < out_tiles)
        def _():
            load_out(c + 4).start()

    lax.fori_loop(0, out_tiles, out, None)
    add(out_tiles - 1)
    store(out_tiles - 1).start()
    ring.drain()
    lax.fori_loop(0, out_tiles, lambda c, _: store(c).wait(), None)


def layer(x, gain, wq, wk, wv, wo, freq, n):
    own, d = x.shape
    heads, key_heads = wq.shape[1] // HEAD, wk.shape[1] // HEAD
    tile = 512
    state = lambda *s: [pltpu.VMEM(s, jnp.float32)] * 2
    hbm, vmem = pl.BlockSpec(memory_space=pl.ANY), pl.BlockSpec(memory_space=pltpu.VMEM)
    return pl.pallas_call(
        functools.partial(_layer_kernel, n=n),
        name="layer",
        in_specs=[hbm, vmem, hbm, hbm, hbm, hbm, vmem],
        out_specs=hbm,
        out_shape=jax.ShapeDtypeStruct((own, d), jnp.bfloat16),
        scratch_shapes=[
            pltpu.VMEM((key_heads, n, 2 * own, HEAD), jnp.bfloat16),
            pltpu.VMEM((own, HEAD), jnp.float32),
            pltpu.VMEM((own, HEAD), jnp.float32),
            pltpu.VMEM((own, tile), jnp.float32),
            pltpu.VMEM((own, d), jnp.bfloat16),
            pltpu.VMEM((own, d), jnp.bfloat16),
            pltpu.VMEM((2, wo.shape[0], tile), jnp.bfloat16),
            pltpu.VMEM((heads, own, HEAD), jnp.bfloat16),
            pltpu.VMEM((own, heads * HEAD), jnp.bfloat16),
            *state(n * own, 2 * own),
            *state(8, 2 * own),
            *state(HEAD + 8, 2 * own),
            pltpu.VMEM((own, 2 * own), jnp.int32),
            pltpu.SemaphoreType.DMA((2, key_heads, 4)),
            pltpu.SemaphoreType.DMA((2, key_heads, 4)),
            pltpu.SemaphoreType.DMA((8,)),
            pltpu.SemaphoreType.DMA,
            pltpu.SemaphoreType.DMA((d * 2 // tile,)),
        ],
        compiler_params=pltpu.CompilerParams(vmem_limit_bytes=VMEM_LIMIT, collective_id=0, has_side_effects=True),
        cost_estimate=pl.CostEstimate(flops=4 * own * d * heads * HEAD, bytes_accessed=4 * d * heads * HEAD, transcendentals=0),
    )(x, jnp.broadcast_to(gain.astype(jnp.float32), (8, d)), wq, wk, wv, wo, freq)


def solution(mesh):
    n = mesh.shape["sp"]

    def step(x, gain, wq, wk, wv, wo):
        half = HEAD // 2
        power = lax.rem(lax.broadcasted_iota(jnp.int32, (8, HEAD), 1), half).astype(jnp.float32)
        return layer(x, gain, wq, wk, wv, wo, THETA ** (-power / half), n)

    tokens, whole = P(("dp", "sp"), None), P(None, None)
    return jax.shard_map(
        step, mesh=mesh, in_specs=(tokens, P(None), whole, whole, whole, whole), out_specs=tokens, check_vma=False)
```
